32 devices in a mesh: data: 1 (over z), dap2: 4 (over y), dap: 8 (over x, core).
Axes of the slice: x: 4, y: 4, z: 1, core: 2. Of those that a mesh axis runs over, the one named last changes fastest.
The devices are a block of a 4x4x8 slice.
Arguments:
- pair_rep: float32 [512, 512, 128], P(('data', 'dap2', 'dap'))
- pair_mask: int32 [512, 512], P(('data', 'dap2', 'dap'))
- norm_gain: bfloat16 [2, 128], replicated
- norm_bias: bfloat16 [2, 128], replicated
- w_proj: bfloat16 [2, 128, 512], replicated
- w_gate: bfloat16 [2, 128, 128], replicated
- post_gain: bfloat16 [2, 128], replicated
- post_bias: bfloat16 [2, 128], replicated
- w_out: bfloat16 [2, 128, 128], replicated
Outputs:
- output: float32 [512, 512, 128], P(('data', 'dap2', 'dap'))
All inputs are finite; a program needn't handle non-finite values.
Results may differ from the reference program's by a relative error of at most 0.00136737.
Values are sent between devices in bfloat16 or wider.
A program may use at most 768 MiB of HBM per device.

```python
import jax
import jax.numpy as jnp
from jax import lax

N = 512
CZ = 128
C = 128
ROW_BLOCKS = 8
BLOCK_ROWS = N // ROW_BLOCKS
NORM_EPS = 1e-5


def setup_inputs(seed: int = 0, part: int = 0) -> dict:
    part_key = jax.random.fold_in(jax.random.key(seed), part)
    pair_key, length_key = jax.random.split(part_key, 2)
    pair_rep = jax.random.normal(pair_key, (N, N, CZ), jnp.float32)
    length = jax.random.randint(length_key, (), N - N // 8, N - N // 16 + 1)
    valid_rows = jnp.arange(N) < length
    pair_mask = (valid_rows[:, None] & valid_rows[None, :]).astype(jnp.int32)
    param_keys = jax.random.split(jax.random.key(seed + 1), 7)
    norm_gain = 1.0 + 0.3 * jax.random.normal(param_keys[0], (2, CZ), jnp.float32)
    norm_bias = 0.3 * jax.random.normal(param_keys[1], (2, CZ), jnp.float32)
    w_proj = jax.random.normal(param_keys[2], (2, CZ, 4 * C), jnp.float32) * CZ ** -0.5
    w_gate = jax.random.normal(param_keys[3], (2, CZ, CZ), jnp.float32) * CZ ** -0.5
    post_gain = 1.0 + 0.3 * jax.random.normal(param_keys[4], (2, C), jnp.float32)
    post_bias = 0.3 * jax.random.normal(param_keys[5], (2, C), jnp.float32)
    w_out = jax.random.normal(param_keys[6], (2, C, CZ), jnp.float32) * (2.0 * C ** -0.5)
    return {
        'pair_rep': pair_rep,
        'pair_mask': pair_mask,
        'norm_gain': norm_gain.astype(jnp.bfloat16),
        'norm_bias': norm_bias.astype(jnp.bfloat16),
        'w_proj': w_proj.astype(jnp.bfloat16),
        'w_gate': w_gate.astype(jnp.bfloat16),
        'post_gain': post_gain.astype(jnp.bfloat16),
        'post_bias': post_bias.astype(jnp.bfloat16),
        'w_out': w_out.astype(jnp.bfloat16),
    }


def layer_norm(values, scale_vec, shift_vec, norm_axis):
    row_mean = jnp.mean(values, axis=norm_axis, keepdims=True)
    centered = values - row_mean
    row_var = jnp.mean(centered * centered, axis=norm_axis, keepdims=True)
    scaled = centered * lax.rsqrt(row_var + NORM_EPS)
    return (scaled * scale_vec.astype(jnp.float32) + shift_vec.astype(jnp.float32)).astype(jnp.bfloat16)


def gated_side(normed, w_pair, keep_blk):
    projected = jnp.dot(normed.reshape(-1, CZ), w_pair, preferred_element_type=jnp.float32)
    projected = projected.reshape(BLOCK_ROWS, N, 2 * C)
    return (keep_blk[..., None] * jax.nn.sigmoid(projected[..., C:]) * projected[..., :C]).astype(jnp.bfloat16)


def outgoing_mix(pair_in):
    return jnp.dot(pair_in[0], pair_in[1].T, preferred_element_type=jnp.float32)


def incoming_mix(pair_in):
    return jnp.dot(pair_in[0].T, pair_in[1], preferred_element_type=jnp.float32)


def tri_update(pair_rep, keep_mask, norm_gain, norm_bias, w_proj, w_gate, post_gain, post_bias, w_out, mix_fn):
    pair_blocks = pair_rep.reshape(ROW_BLOCKS, BLOCK_ROWS, N, CZ)
    keep_blocks = keep_mask.reshape(ROW_BLOCKS, BLOCK_ROWS, N)

    def project(block_in):
        pair_blk, keep_blk = block_in
        normed = layer_norm(pair_blk, norm_gain, norm_bias, -1)
        return (gated_side(normed, w_proj[:, :2 * C], keep_blk),
                gated_side(normed, w_proj[:, 2 * C:], keep_blk))

    side_a, side_b = lax.map(project, (pair_blocks, keep_blocks))
    chan_a = jnp.moveaxis(side_a.reshape(N, N, C), 2, 0)
    chan_b = jnp.moveaxis(side_b.reshape(N, N, C), 2, 0)
    mixed_sum = lax.map(mix_fn, (chan_a, chan_b))
    mixed_blocks = jnp.moveaxis(mixed_sum.reshape(C, ROW_BLOCKS, BLOCK_ROWS, N), 1, 0)

    def finish(block_in):
        pair_blk, mixed_blk = block_in
        normed = layer_norm(pair_blk, norm_gain, norm_bias, -1)
        post_norm = layer_norm(mixed_blk, post_gain[:, None, None], post_bias[:, None, None], 0)
        update = jnp.dot(jnp.moveaxis(post_norm, 0, -1).reshape(-1, C), w_out, preferred_element_type=jnp.float32)
        gate_pre = jnp.dot(normed.reshape(-1, CZ), w_gate, preferred_element_type=jnp.float32)
        gated_out = jax.nn.sigmoid(gate_pre) * update
        return pair_blk + gated_out.reshape(BLOCK_ROWS, N, CZ)

    return lax.map(finish, (pair_blocks, mixed_blocks)).reshape(N, N, CZ)


def reference(pair_rep, pair_mask, norm_gain, norm_bias, w_proj, w_gate, post_gain, post_bias, w_out):
    keep_mask = pair_mask.astype(jnp.float32)
    pair_mid = tri_update(pair_rep, keep_mask, norm_gain[0], norm_bias[0], w_proj[0], w_gate[0],
                          post_gain[0], post_bias[0], w_out[0], outgoing_mix)
    return tri_update(pair_mid, keep_mask, norm_gain[1], norm_bias[1], w_proj[1], w_gate[1],
                      post_gain[1], post_bias[1], w_out[1], incoming_mix)
```

```python
import functools

import jax
import jax.numpy as jnp
from jax import lax
from jax.experimental import pallas as pl
from jax.experimental.pallas import tpu as pltpu
from jax.sharding import PartitionSpec as P

NORM_EPS = 1e-5
ROW_SPEC = P(('data', 'dap2', 'dap'), None, None)
MASK_SPEC = P(('data', 'dap2', 'dap'), None)
MESH = pl.DeviceIdType.MESH
F32, BF16 = jnp.float32, jnp.bfloat16
CORES = 2
LANES = 128
PAD = 8


def norm(values, gain, bias, axis):
    mean = jnp.mean(values, axis=axis, keepdims=True)
    centered = values - mean
    var = jnp.mean(centered * centered, axis=axis, keepdims=True)
    return (centered * lax.rsqrt(var + NORM_EPS) * gain + bias).astype(BF16)


def dot(a, b, ca, cb):
    return lax.dot_general(a, b, (((ca,), (cb,)), ((), ())), preferred_element_type=F32)


def update_kernel(ny, nx, incoming, z_ref, mask_ref, ng_ref, nb_ref, wp_ref, wg_ref, pg_ref, pb_ref, wo_ref, out_ref,
                  yn_ref, sa_ref, sb_ref, ab_ref, t_ref, r_ref, x_ref, u_ref, xr_ref,
                  p1s, p1r, p2s, p2r, x1s, x1r, x2s, x2r):
    rows, n, ch = z_ref.shape
    nt = n // LANES
    y = lax.axis_index('dap2')
    d = lax.axis_index('dap')
    x, c = d // CORES, d % CORES
    size1, size2 = (nx, ny), (ny, nx)
    pos1, pos2 = (x, y), (y, x)

    def peer(s, first, place, core):
        on_x = (s == 0) == first
        return {'dap2': y, 'dap': place * CORES + core} if on_x else {'dap2': place, 'dap': x * CORES + core}

    barrier = pltpu.get_barrier_semaphore()
    greeted = 0
    for on_x, size, pos in ((True, nx, x), (False, ny, y)):
        for o in range(size):
            for oc in range(CORES):
                if (o, oc) == (0, 0) or (o == 0 and not on_x):
                    continue
                pl.semaphore_signal(barrier, inc=1, device_id=peer(0, on_x, (pos + o) % size, (c + oc) % CORES),
                                    device_id_type=MESH)
                greeted += 1

    gain, bias = ng_ref[...].astype(F32), nb_ref[...].astype(F32)
    step = 2 * LANES
    spad = ch + PAD

    @pl.loop(0, rows)
    def _(i):
        yn = norm(z_ref[i], gain, bias, -1)
        yn_ref[i] = yn
        for kb in range(n // step):
            keep = mask_ref[pl.ds(i, 1), kb * step:(kb + 1) * step].astype(F32)
            ynk = yn[kb * step:(kb + 1) * step]
            for side, dst in ((0, sa_ref), (1, sb_ref)):
                w = wp_ref[side * 2 * ch:(side + 1) * 2 * ch]
                pr = dot(w, ynk, 1, 1)
                val = keep * jax.nn.sigmoid(pr[ch:]) * pr[:ch]
                for t in range(2):
                    dst[kb * 2 + t, pl.ds(pl.multiple_of(i * spad, 8), ch)] = val[:, t * LANES:(t + 1) * LANES]

    abf = ab_ref.reshape(2, ch, rows, n)

    @pl.loop(0, ch)
    def _(k):
        for side, src in ((0, sa_ref), (1, sb_ref)):
            for t in range(nt):
                abf[side, k, :, t * LANES:(t + 1) * LANES] = src[t, pl.ds(k, rows, stride=spad)].astype(BF16)

    pl.semaphore_wait(barrier, greeted)

    def send(src, dst, ss, rs, dev):
        cp = pltpu.make_async_remote_copy(src_ref=src, dst_ref=dst, send_sem=ss, recv_sem=rs, device_id=dev,
                                          device_id_type=MESH)
        cp.start()
        return cp

    sent = []
    hop1, hop2, back1, back2 = {}, {}, {}, {}
    rounds = [(r, s) for r in range(2) for s in range(2)]
    for r, s in rounds:
        hop1[r, s] = []
        for o in range(1, size1[s]):
            g = (pos1[s] + o) % size1[s]
            hop1[r, s].append(send(ab_ref.at[:, s, g, :, r], t_ref.at[s, :, :, r, pos1[s]], p1s.at[s, r, o],
                                   p1r.at[s, r, o], peer(s, True, g, c)))
    for r, s in rounds:
        t_ref[s, :, :, r, pos1[s]] = ab_ref[:, s, pos1[s], :, r]
    for r, s in rounds:
        for cp in hop1[r, s]:
            cp.wait_recv()
        hop2[r, s] = []
        for o in range(size2[s]):
            h = (pos2[s] + o) % size2[s]
            for oc in range(CORES):
                k = (c + oc) % CORES
                src = t_ref.at[s, :, h * CORES + k, r]
                dst = r_ref.at[:, s, r, y, :, c] if s == 0 else r_ref.at[:, s, r, :, x, c]
                if (o, oc) != (0, 0):
                    hop2[r, s].append(send(src, dst, p2s.at[s, r, o * CORES + oc], p2r.at[s, r, o * CORES + oc],
                                           peer(s, False, h, k)))
        own = t_ref[s, :, pos2[s] * CORES + c, r]
        if s == 0:
            r_ref[:, s, r, y, :, c] = own
        else:
            r_ref[:, s, r, :, x, c] = own
    blk = 2 * LANES
    rf = r_ref.reshape(2, 2, 2, n, n)
    xf = x_ref.reshape(2, 2, n // rows, nt * rows, LANES)
    for r, s in rounds:
        for cp in hop2[r, s]:
            cp.wait_recv()
        for ib in range(n // blk):
            for jb in range(n // blk):
                isl, jsl = slice(ib * blk, (ib + 1) * blk), slice(jb * blk, (jb + 1) * blk)
                if incoming:
                    prod = dot(rf[0, s, r, :, isl], rf[1, s, r, :, jsl], 0, 0)
                else:
                    prod = dot(rf[0, s, r, isl], rf[1, s, r, jsl], 1, 1)
                for t in range(2):
                    q = jb * 2 + t
                    xf[s, r, ib * (blk // rows):(ib + 1) * (blk // rows), q * rows:(q + 1) * rows, :] = (
                        prod[:, t * LANES:(t + 1) * LANES].reshape(blk // rows, rows, LANES))
        back1[r, s] = []
        for o in range(1, size2[s]):
            h = (pos2[s] + o) % size2[s]
            src = x_ref.at[s, r, h] if s == 0 else x_ref.at[s, r, :, h]
            back1[r, s].append(send(src, u_ref.at[s, :, :, pos2[s], r], x1s.at[s, r, o], x1r.at[s, r, o],
                                    peer(s, False, h, c)))
        u_ref[s, :, :, pos2[s], r] = x_ref[s, r, y] if s == 0 else x_ref[s, r, :, x]
    for r, s in rounds:
        for cp in back1[r, s]:
            cp.wait_recv()
        back2[r, s] = []
        for o in range(size1[s]):
            g = (pos1[s] + o) % size1[s]
            for oc in range(CORES):
                k = (c + oc) % CORES
                if (o, oc) != (0, 0):
                    back2[r, s].append(send(u_ref.at[s, g, k, :, r],
                                            xr_ref.at[s, pos1[s], :, c, r, pl.ds(0, nt * rows)],
                                            x2s.at[s, r, o * CORES + oc], x2r.at[s, r, o * CORES + oc],
                                            peer(s, True, g, k)))
        xr_ref[s, pos1[s], :, c, r, pl.ds(0, nt * rows)] = u_ref[s, pos1[s], c, :, r]
    for key in rounds:
        for cp in back2[key]:
            cp.wait_recv()

    pgain, pbias = pg_ref[...].astype(F32), pb_ref[...].astype(F32)
    xpad = nt * rows + PAD
    xrf = xr_ref.reshape(ch * xpad, LANES)

    @pl.loop(0, rows)
    def _(i):
        for t in range(nt):
            js = slice(t * LANES, (t + 1) * LANES)
            xn = norm(xrf[pl.ds(t * rows + i, ch, stride=xpad)], pgain, pbias, 0)
            upd = dot(xn, wo_ref[...], 0, 0)
            pre = dot(yn_ref[i, js], wg_ref[...], 1, 0)
            out_ref[i, js] = z_ref[i, js] + jax.nn.sigmoid(pre) * upd

    for group in (hop1, hop2, back1, back2):
        for key in rounds:
            for cp in group[key]:
                cp.wait_send()


def update(ny, nx, incoming, pair, mask, ng, nb, wp, wg, pg, pb, wo):
    rows, n, ch = pair.shape
    nt = n // LANES
    per = ch // (ny * nx * CORES * 2)
    assert per == 2 and ny == nx
    vmem = pl.BlockSpec(memory_space=pltpu.VMEM)
    dma = pltpu.SemaphoreType.DMA
    g = nx
    return pl.pallas_call(
        functools.partial(update_kernel, ny, nx, incoming),
        name='incoming' if incoming else 'outgoing',
        out_shape=jax.ShapeDtypeStruct(pair.shape, F32),
        in_specs=[vmem] * 9,
        out_specs=vmem,
        scratch_shapes=[
            pltpu.VMEM((rows, n, ch), BF16),
            pltpu.VMEM((nt, rows * (ch + PAD), LANES), F32),
            pltpu.VMEM((nt, rows * (ch + PAD), LANES), F32),
            pltpu.VMEM((2, 2, g, g * CORES, 2, rows, n), BF16),
            pltpu.VMEM((2, 2, g * CORES, 2, g, rows, n), BF16),
            pltpu.VMEM((2, 2, 2, ny, nx, CORES, rows, n), BF16),
            pltpu.VMEM((2, 2, ny, nx, CORES, nt * rows, LANES), F32),
            pltpu.VMEM((2, g, CORES, g, 2, nt * rows, LANES), F32),
            pltpu.VMEM((2, g, g, CORES, 2, nt * rows + PAD, LANES), F32),
            dma((2, 2, g)), dma((2, 2, g)), dma((2, 2, g * CORES)), dma((2, 2, g * CORES)),
            dma((2, 2, g)), dma((2, 2, g)), dma((2, 2, g * CORES)), dma((2, 2, g * CORES)),
        ],
        compiler_params=pltpu.CompilerParams(collective_id=1 if incoming else 0, has_side_effects=True,
                                             vmem_limit_bytes=60 * 2 ** 20),
    )(pair, mask, ng, nb, wp, wg, pg, pb, wo)


def solution(mesh):
    ny, nx = mesh.shape['dap2'], mesh.shape['dap'] // CORES

    def local_step(pair, mask, norm_gain, norm_bias, w_proj, w_gate, post_gain, post_bias, w_out):
        for s in range(2):
            pair = update(ny, nx, s == 1, pair, mask, norm_gain[s][None], norm_bias[s][None], w_proj[s].T, w_gate[s],
                          post_gain[s][:, None], post_bias[s][:, None], w_out[s])
        return pair

    return jax.shard_map(local_step, mesh=mesh, in_specs=(ROW_SPEC, MASK_SPEC) + (P(),) * 7, out_specs=ROW_SPEC,
                         check_vma=False)
```

```python
import functools

import jax
import jax.numpy as jnp
from jax import lax
from jax.experimental import pallas as pl
from jax.experimental.pallas import tpu as pltpu
from jax.sharding import PartitionSpec as P

NORM_EPS = 1e-5
ROW_SPEC = P(('data', 'dap2', 'dap'), None, None)
MASK_SPEC = P(('data', 'dap2', 'dap'), None)
MESH = pl.DeviceIdType.MESH
F32, BF16 = jnp.float32, jnp.bfloat16
CORES = 2
LANES = 128
PAD = 8
HALVES = 2


def norm(values, gain, bias, axis):
    mean = jnp.mean(values, axis=axis, keepdims=True)
    centered = values - mean
    var = jnp.mean(centered * centered, axis=axis, keepdims=True)
    return (centered * lax.rsqrt(var + NORM_EPS) * gain + bias).astype(BF16)


def dot(a, b, ca, cb):
    return lax.dot_general(a, b, (((ca,), (cb,)), ((), ())), preferred_element_type=F32)


def both_updates(ny, nx, z_hbm, mask_ref, ng_ref, nb_ref, wp_ref, wg_ref, pg_ref, pb_ref, wo_ref, out_hbm,
                 z_ref, yn_ref, wt_ref, gb_ref, st_ref, ab_ref, t_ref, r_ref, x_ref, u_ref, xr_ref,
                 ssem, rsem, zsem):
    rows, n, ch = z_ref.shape
    width = n // HALVES
    nt = width // LANES
    xrows = nt * rows
    spad = ch + PAD
    xpad = HALVES * xrows + PAD
    y = lax.axis_index('dap2')
    d = lax.axis_index('dap')
    x, c = d // CORES, d % CORES
    size1, size2 = (nx, ny), (ny, nx)
    pos1, pos2 = (x, y), (y, x)
    blocks = ny * nx * CORES

    loads = []
    for q in range(HALVES):
        cols = pl.ds(q * width, width)
        loads.append(pltpu.make_async_copy(z_hbm.at[:, cols], z_ref.at[:, cols], zsem.at[0, q]))
        loads[q].start()

    def peer(s, first, place, core):
        on_x = (s == 0) == first
        return {'dap2': y, 'dap': place * CORES + core} if on_x else {'dap2': place, 'dap': x * CORES + core}

    barrier = pltpu.get_barrier_semaphore()
    greeted = 0
    for on_x, size, pos in ((True, nx, x), (False, ny, y)):
        for o in range(size):
            for oc in range(CORES):
                if (o, oc) == (0, 0) or (o == 0 and not on_x):
                    continue
                pl.semaphore_signal(barrier, inc=1, device_id=peer(0, on_x, (pos + o) % size, (c + oc) % CORES),
                                    device_id_type=MESH)
                greeted += 1

    for u in range(2):
        wt_ref[u] = wp_ref[u].T
        gb_ref[u, 0] = jnp.broadcast_to(pg_ref[u:u + 1].astype(F32), (LANES, ch)).T
        gb_ref[u, 1] = jnp.broadcast_to(pb_ref[u:u + 1].astype(F32), (LANES, ch)).T

    abf = ab_ref.reshape(2, ch, rows, n)
    rf = r_ref.reshape(2, 2, 2, 2, n, n)
    rw = r_ref.reshape(2, 2, 2, 2, blocks, rows, n)
    xf = x_ref.reshape(2, 2, blocks, HALVES * xrows, LANES)
    xrf = xr_ref.reshape(2 * ch * xpad, LANES)

    def finish_row(u, q, i):
        for t in range(nt):
            js = slice(q * width + t * LANES, q * width + (t + 1) * LANES)
            xn = norm(xrf[pl.ds(u * ch * xpad + (q * nt + t) * rows + i, ch, stride=xpad)], gb_ref[u, 0], gb_ref[u, 1], 0)
            upd = dot(xn, wo_ref[u], 0, 0)
            pre = dot(yn_ref[i, js], wg_ref[u], 1, 0)
            z_ref[i, js] = z_ref[i, js] + jax.nn.sigmoid(pre) * upd

    def project_row(u, q, i):
        js = slice(q * width, (q + 1) * width)
        yn = norm(z_ref[i, js], ng_ref[u:u + 1].astype(F32), nb_ref[u:u + 1].astype(F32), -1)
        yn_ref[i, js] = yn
        keep = mask_ref[pl.ds(i, 1), js].astype(F32)
        for side in range(2):
            pr = dot(wt_ref[u, side * 2 * ch:(side + 1) * 2 * ch], yn, 1, 1)
            val = keep * jax.nn.sigmoid(pr[ch:]) * pr[:ch]
            for t in range(nt):
                st_ref[side, t, pl.ds(pl.multiple_of(i * spad, 8), ch)] = val[:, t * LANES:(t + 1) * LANES]

    def repack(q):
        @pl.loop(0, ch)
        def _(k):
            for side in range(2):
                for t in range(nt):
                    lanes = slice(q * width + t * LANES, q * width + (t + 1) * LANES)
                    abf[side, k, :, lanes] = st_ref[side, t, pl.ds(k, rows, stride=spad)].astype(BF16)

    def send(src, dst, where, dev):
        pltpu.make_async_remote_copy(src_ref=src, dst_ref=dst, send_sem=ssem.at[where], recv_sem=rsem.at[where],
                                     device_id=dev, device_id_type=MESH).start()

    def wait(sem, view):
        pltpu.make_async_copy(view, view, sem).wait()

    HOP1, HOP2, BACK1, BACK2 = range(4)
    cols = [slice(q * width, (q + 1) * width) for q in range(HALVES)]
    xcols = [slice(q * xrows, (q + 1) * xrows) for q in range(HALVES)]

    def view(stage, u, q, r, s):
        if stage == HOP1:
            return t_ref.at[u, s, :, :, r, 0:size1[s] - 1, :, cols[q]]
        if stage == HOP2:
            return rw.at[u, :, s, r, 0:blocks - blocks // (size2[s] * CORES), :, cols[q]]
        if stage == BACK1:
            return xf.at[s, r, 0:blocks - blocks // size2[s], xcols[q]]
        return xf.at[s, r, 0:blocks - blocks // (size1[s] * CORES), xcols[q]]

    def arrived(stage, u, q, r):
        for s in range(2):
            wait(rsem.at[stage, u, q, r, s], view(stage, u, q, r, s))

    def left(stage, u):
        for q in range(HALVES):
            for r in range(2):
                for s in range(2):
                    wait(ssem.at[stage, u, q, r, s], view(stage, u, q, r, s))

    def hop1(u, q, r):
        for o in range(1, nx):
            for s in range(2):
                g = (pos1[s] + o) % size1[s]
                send(ab_ref.at[:, s, g, :, r, :, cols[q]], t_ref.at[u, s, :, :, r, pos1[s], :, cols[q]],
                     (HOP1, u, q, r, s), peer(s, True, g, c))
        for s in range(2):
            t_ref[u, s, :, :, r, pos1[s], :, cols[q]] = ab_ref[:, s, pos1[s], :, r, :, cols[q]]

    def hop2(u, q, r):
        arrived(HOP1, u, q, r)
        for o in range(ny):
            for oc in range(CORES):
                for s in range(2):
                    h, k = (pos2[s] + o) % size2[s], (c + oc) % CORES
                    src = (u, s, slice(None), h * CORES + k, r, slice(None), slice(None), cols[q])
                    dst = (u, slice(None), s, r) + ((y, slice(None)) if s == 0 else (slice(None), x)) + (
                        c, slice(None), cols[q])
                    if (o, oc) == (0, 0):
                        r_ref[dst] = t_ref[src]
                    else:
                        send(t_ref.at[src], r_ref.at[dst], (HOP2, u, q, r, s), peer(s, False, h, k))

    def product(u, r):
        blk = 2 * LANES
        for s in range(2):
            for ib in range(n // blk):
                for jb in range(n // blk):
                    isl, jsl = slice(ib * blk, (ib + 1) * blk), slice(jb * blk, (jb + 1) * blk)
                    if u == 1:
                        prod = dot(rf[u, 0, s, r, :, isl], rf[u, 1, s, r, :, jsl], 0, 0)
                    else:
                        prod = dot(rf[u, 0, s, r, isl], rf[u, 1, s, r, jsl], 1, 1)
                    per = blk // rows
                    for t in range(2):
                        w = jb * 2 + t
                        xf[s, r, ib * per:(ib + 1) * per, w * rows:(w + 1) * rows, :] = (
                            prod[:, t * LANES:(t + 1) * LANES].reshape(per, rows, LANES))

    def back1(u, q, r):
        for o in range(1, ny):
            for s in range(2):
                h = (pos2[s] + o) % size2[s]
                src = x_ref.at[s, r, h, :, :, xcols[q]] if s == 0 else x_ref.at[s, r, :, h, :, xcols[q]]
                send(src, u_ref.at[u, s, :, :, pos2[s], r, xcols[q]], (BACK1, u, q, r, s), peer(s, False, h, c))
        for s in range(2):
            u_ref[u, s, :, :, pos2[s], r, xcols[q]] = x_ref[s, r, y, :, :, xcols[q]] if s == 0 else (
                x_ref[s, r, :, x, :, xcols[q]])

    def back2(u, q, r):
        arrived(BACK1, u, q, r)
        for o in range(nx):
            for oc in range(CORES):
                for s in range(2):
                    g, k = (pos1[s] + o) % size1[s], (c + oc) % CORES
                    src, dst = (u, s, g, k, slice(None), r, xcols[q]), (u, s, pos1[s], slice(None), c, r, xcols[q])
                    if (o, oc) == (0, 0):
                        xr_ref[dst] = u_ref[src]
                    else:
                        send(u_ref.at[src], xr_ref.at[dst], (BACK2, u, q, r, s), peer(s, True, g, k))

    stores = []
    for u in range(3):
        for q in range(HALVES):
            if u > 0:
                for r in range(2):
                    arrived(BACK2, u - 1, q, r)
            else:
                loads[q].wait()
            if u == 1 and q == 0:
                left(HOP1, 0)

            @pl.loop(0, rows)
            def _(i):
                if u > 0:
                    finish_row(u - 1, q, i)
                if u < 2:
                    project_row(u, q, i)

            if u == 2:
                c_ = pl.ds(q * width, width)
                stores.append(pltpu.make_async_copy(z_ref.at[:, c_], out_hbm.at[:, c_], zsem.at[1, q]))
                stores[q].start()
                continue
            repack(q)
            if u == 0 and q == 0:
                pl.semaphore_wait(barrier, greeted)
            for r in range(2):
                hop1(u, q, r)
        if u == 2:
            break
        for q in range(HALVES):
            for r in range(2):
                hop2(u, q, r)
        if u == 1:
            left(BACK1, 0)
        for r in range(2):
            for q in range(HALVES):
                arrived(HOP2, u, q, r)
            product(u, r)
            back1(u, 0, r)
        for q in range(1, HALVES):
            for r in range(2):
                back1(u, q, r)
        for q in range(HALVES):
            for r in range(2):
                back2(u, q, r)
    for stage, u in ((HOP1, 1), (HOP2, 0), (HOP2, 1), (BACK1, 1), (BACK2, 0), (BACK2, 1)):
        left(stage, u)
    for q in range(HALVES):
        stores[q].wait()


def solution(mesh):
    ny, nx = mesh.shape['dap2'], mesh.shape['dap'] // CORES
    assert ny == nx
    g = nx

    def local_step(pair, mask, norm_gain, norm_bias, w_proj, w_gate, post_gain, post_bias, w_out):
        rows, n, ch = pair.shape
        nt = n // LANES
        assert ch == g * g * CORES * 4 and ch == LANES
        vmem = pl.BlockSpec(memory_space=pltpu.VMEM)
        hbm = pl.BlockSpec(memory_space=pl.ANY)
        dma = pltpu.SemaphoreType.DMA
        return pl.pallas_call(
            functools.partial(both_updates, ny, nx),
            name='triangle',
            out_shape=jax.ShapeDtypeStruct(pair.shape, F32),
            in_specs=[hbm] + [vmem] * 8,
            out_specs=hbm,
            scratch_shapes=[
                pltpu.VMEM((rows, n, ch), F32),
                pltpu.VMEM((rows, n, ch), BF16),
                pltpu.VMEM((2, 4 * ch, ch), BF16),
                pltpu.VMEM((2, 2, ch, LANES), F32),
                pltpu.VMEM((2, nt // HALVES, rows * (ch + PAD), LANES), F32),
                pltpu.VMEM((2, 2, g, g * CORES, 2, rows, n), BF16),
                pltpu.VMEM((2, 2, 2, g * CORES, 2, g, rows, n), BF16),
                pltpu.VMEM((2, 2, 2, 2, ny, nx, CORES, rows, n), BF16),
                pltpu.VMEM((2, 2, ny, nx, CORES, nt * rows, LANES), F32),
                pltpu.VMEM((2, 2, g, CORES, g, 2, nt * rows, LANES), F32),
                pltpu.VMEM((2, 2, g, g, CORES, 2, nt * rows + PAD, LANES), F32),
                dma((4, 2, HALVES, 2, 2)), dma((4, 2, HALVES, 2, 2)), dma((2, HALVES)),
            ],
            compiler_params=pltpu.CompilerParams(collective_id=0, has_side_effects=True,
                                                 vmem_limit_bytes=63 * 2 ** 20),
        )(pair, mask, norm_gain, norm_bias, w_proj, w_gate, post_gain, post_bias, w_out)

    return jax.shard_map(local_step, mesh=mesh, in_specs=(ROW_SPEC, MASK_SPEC) + (P(),) * 7, out_specs=ROW_SPEC,
                         check_vma=False)
```

```python
import functools

import jax
import jax.numpy as jnp
from jax import lax
from jax.experimental import pallas as pl
from jax.experimental.pallas import tpu as pltpu
from jax.sharding import PartitionSpec as P

NORM_EPS = 1e-5
ROW_SPEC = P(('data', 'dap2', 'dap'), None, None)
MASK_SPEC = P(('data', 'dap2', 'dap'), None)
MESH = pl.DeviceIdType.MESH
F32, BF16 = jnp.float32, jnp.bfloat16
CORES = 2
LANES = 128
PAD = 8
HALVES = 2
RING = 4


def norm(values, gain, bias, axis):
    mean = jnp.mean(values, axis=axis, keepdims=True)
    centered = values - mean
    var = jnp.mean(centered * centered, axis=axis, keepdims=True)
    return (centered * lax.rsqrt(var + NORM_EPS) * gain + bias).astype(BF16)


def dot(a, b, ca, cb):
    return lax.dot_general(a, b, (((ca,), (cb,)), ((), ())), preferred_element_type=F32)


def both_updates(ny, nx, z_hbm, mask_ref, ng_ref, nb_ref, wp_ref, wg_ref, pg_ref, pb_ref, wo_ref, out_hbm,
                 z_ref, yn_ref, wt_ref, gb_ref, st_ref, ab_ref, a0_ref, b0_ref, t_ref, r_ref, x_ref, u_ref, xr_ref,
                 ssem, rsem, zsem):
    rows, n, ch = z_ref.shape
    width = n // HALVES
    nt = width // LANES
    xrows = nt * rows
    spad = ch + PAD
    xpad = HALVES * xrows + PAD
    y = lax.axis_index('dap2')
    d = lax.axis_index('dap')
    x, c = d // CORES, d % CORES
    size1, size2 = (nx, ny), (ny, nx)
    pos1, pos2 = (x, y), (y, x)
    blocks = ny * nx * CORES

    loads = []
    for q in range(HALVES):
        cols = pl.ds(q * width, width)
        loads.append(pltpu.make_async_copy(z_hbm.at[:, cols], z_ref.at[:, cols], zsem.at[0, q]))
        loads[q].start()

    def peer(s, first, place, core):
        on_x = (s == 0) == first
        return {'dap2': y, 'dap': place * CORES + core} if on_x else {'dap2': place, 'dap': x * CORES + core}

    barrier = pltpu.get_barrier_semaphore()
    greeted = 0
    for on_x, size, pos in ((True, nx, x), (False, ny, y)):
        for o in range(size):
            for oc in range(CORES):
                if (o, oc) == (0, 0) or (o == 0 and not on_x):
                    continue
                pl.semaphore_signal(barrier, inc=1, device_id=peer(0, on_x, (pos + o) % size, (c + oc) % CORES),
                                    device_id_type=MESH)
                greeted += 1

    for u in range(2):
        wt_ref[u] = wp_ref[u].T
        gb_ref[u, 0] = jnp.broadcast_to(pg_ref[u:u + 1].astype(F32), (LANES, ch)).T
        gb_ref[u, 1] = jnp.broadcast_to(pb_ref[u:u + 1].astype(F32), (LANES, ch)).T

    abf = ab_ref.reshape(2, ch, rows, n)
    rf = r_ref.reshape(2, 2, 2, n, n)
    rw = r_ref.reshape(2, 2, 2, blocks, rows, n)
    band = nx * CORES
    per0 = ch // (2 * band)
    part = per0 // 2
    ab0 = ab_ref.reshape(2, 2, nx, CORES, per0, rows, n)
    a0f = a0_ref.reshape(2, per0, band * rows, n)
    b0f = b0_ref.reshape(2, per0, n, n)
    x0 = x_ref.reshape(2, per0, band, HALVES * xrows, LANES)
    xr0 = xr_ref.reshape(2, 2, nx, CORES, per0, xpad, LANES)
    xf = x_ref.reshape(2, 2, blocks, HALVES * xrows, LANES)
    xrf = xr_ref.reshape(2 * ch * xpad, LANES)

    def finish_row(u, q, i):
        for t in range(nt):
            js = slice(q * width + t * LANES, q * width + (t + 1) * LANES)
            xn = norm(xrf[pl.ds(u * ch * xpad + (q * nt + t) * rows + i, ch, stride=xpad)], gb_ref[u, 0], gb_ref[u, 1], 0)
            upd = dot(xn, wo_ref[u], 0, 0)
            pre = dot(yn_ref[i, js], wg_ref[u], 1, 0)
            z_ref[i, js] = z_ref[i, js] + jax.nn.sigmoid(pre) * upd

    def project_row(u, q, i):
        js = slice(q * width, (q + 1) * width)
        yn = norm(z_ref[i, js], ng_ref[u:u + 1].astype(F32), nb_ref[u:u + 1].astype(F32), -1)
        yn_ref[i, js] = yn
        keep = mask_ref[pl.ds(i, 1), js].astype(F32)
        for side in range(2):
            pr = dot(wt_ref[u, side * 2 * ch:(side + 1) * 2 * ch], yn, 1, 1)
            val = keep * jax.nn.sigmoid(pr[ch:]) * pr[:ch]
            for t in range(nt):
                st_ref[side, t, pl.ds(pl.multiple_of(i * spad, 8), ch)] = val[:, t * LANES:(t + 1) * LANES]

    def repack(q):
        @pl.loop(0, ch, unroll=8)
        def _(k):
            for side in range(2):
                for t in range(nt):
                    lanes = slice(q * width + t * LANES, q * width + (t + 1) * LANES)
                    abf[side, k, :, lanes] = st_ref[side, t, pl.ds(k, rows, stride=spad)].astype(BF16)

    def send(src, dst, where, dev):
        pltpu.make_async_remote_copy(src_ref=src, dst_ref=dst, send_sem=ssem.at[where], recv_sem=rsem.at[where],
                                     device_id=dev, device_id_type=MESH).start()

    def wait(sem, view):
        pltpu.make_async_copy(view, view, sem).wait()

    HOP1, HOP2, BACK1, BACK2 = range(4)
    cols = [slice(q * width, (q + 1) * width) for q in range(HALVES)]
    xcols = [slice(q * xrows, (q + 1) * xrows) for q in range(HALVES)]

    def view(stage, u, q, r, s):
        if u == 0:
            if stage == HOP1:
                return abf.at[:, 0:(band - 1) * per0, :, cols[q]]
            if stage == HOP2:
                return b0_ref.at[s, :, 0, :, :, :, cols[q]]
            if stage == BACK1:
                return b0_ref.at[s, 0:part, 0, :, :, :, cols[q]]
            return x0.at[s, 0:part, 0:band - 1, xcols[q]]
        if stage == HOP1:
            return t_ref.at[s, :, :, r, 0:size1[s] - 1, :, cols[q]]
        if stage == HOP2:
            return rw.at[:, s, r, 0:blocks - blocks // (size2[s] * CORES), :, cols[q]]
        if stage == BACK1:
            return xf.at[s, r, 0:blocks - blocks // size2[s], xcols[q]]
        return xf.at[s, r, 0:blocks - blocks // (size1[s] * CORES), xcols[q]]

    def arrived(stage, u, q, r):
        for s in range(2):
            wait(rsem.at[stage, u, q, r, s], view(stage, u, q, r, s))

    def left(stage, u):
        for q in range(HALVES):
            for r in range(1 if (stage, u) == (HOP1, 0) else 2):
                for s in range(2):
                    wait(ssem.at[stage, u, q, r, s], view(stage, u, q, r, s))

    def slab(s, kk, h, q):
        place = (h, slice(None)) if s == 0 else (slice(None), h)
        return (s, kk) + place + (slice(None), slice(None), cols[q])

    def spread(q):
        for o in range(nx):
            for oc in range(CORES):
                for s in range(2):
                    g, k = (pos1[s] + o) % size1[s], (c + oc) % CORES
                    mine = pos1[s] * CORES + c
                    for side, dst, at in ((1, b0_ref, (s, slice(None), y, x, c, slice(None), cols[q])),
                                          (0, a0_ref, (s, slice(None), mine, slice(None), cols[q]))):
                        src = (side, s, g, k, slice(None), slice(None), cols[q])
                        if (o, oc) == (0, 0):
                            dst[at] = ab0[src]
                        else:
                            send(ab0.at[src], dst.at[at], (HOP1, 0, q, 0, s), peer(s, True, g, k))

    def gather(q, r):
        for step in (1, -1):
            for s in range(2):
                at = slab(s, slice(r * part, (r + 1) * part), pos2[s], q)
                send(b0_ref.at[at], b0_ref.at[at], (HOP2, 0, q, r, s), peer(s, False, (pos2[s] + step) % size2[s], c))

    def relay(q, r):
        arrived(HOP2, 0, q, r)
        half = part // 2
        for step, lo in ((1, 0), (-1, half)):
            for s in range(2):
                at = slab(s, slice(r * part + lo, r * part + lo + half), (pos2[s] - step) % size2[s], q)
                send(b0_ref.at[at], b0_ref.at[at], (BACK1, 0, q, r, s), peer(s, False, (pos2[s] + step) % size2[s], c))

    def product0(r):
        for q in range(HALVES):
            arrived(BACK1, 0, q, r)
        blk = 2 * LANES
        for s in range(2):
            for k in range(r * part, (r + 1) * part):
                for jb in range(n // blk):
                    prod = dot(a0f[s, k], b0f[s, k, jb * blk:(jb + 1) * blk], 1, 1)
                    for t in range(2):
                        w = jb * 2 + t
                        x0[s, k, :, w * rows:(w + 1) * rows, :] = (
                            prod[:, t * LANES:(t + 1) * LANES].reshape(band, rows, LANES))

    def give_back(q, r):
        for o in range(nx):
            for oc in range(CORES):
                for s in range(2):
                    g, k = (pos1[s] + o) % size1[s], (c + oc) % CORES
                    kk = slice(r * part, (r + 1) * part)
                    src, dst = (s, kk, g * CORES + k, xcols[q]), (0, s, pos1[s], c, kk, xcols[q])
                    if (o, oc) == (0, 0):
                        xr0[dst] = x0[src]
                    else:
                        send(x0.at[src], xr0.at[dst], (BACK2, 0, q, r, s), peer(s, True, g, k))

    def outgoing():
        for q in range(HALVES):
            arrived(HOP1, 0, q, 0)
            for r in range(2):
                if (q, r) != (HALVES - 1, 1):
                    gather(q, r)
        for q in range(HALVES):
            relay(q, 0)
        gather(HALVES - 1, 1)
        for q in range(HALVES - 1):
            relay(q, 1)
        product0(0)
        relay(HALVES - 1, 1)
        give_back(0, 0)
        product0(1)
        give_back(0, 1)
        for q in range(1, HALVES):
            for r in range(2):
                give_back(q, r)

    def hop1(q, r):
        for o in range(1, nx):
            for s in range(2):
                g = (pos1[s] + o) % size1[s]
                send(ab_ref.at[:, s, g, :, r, :, cols[q]], t_ref.at[s, :, :, r, pos1[s], :, cols[q]],
                     (HOP1, 1, q, r, s), peer(s, True, g, c))
        for s in range(2):
            t_ref[s, :, :, r, pos1[s], :, cols[q]] = ab_ref[:, s, pos1[s], :, r, :, cols[q]]

    def hop2(q, r):
        arrived(HOP1, 1, q, r)
        for o in range(ny):
            for oc in range(CORES):
                for s in range(2):
                    h, k = (pos2[s] + o) % size2[s], (c + oc) % CORES
                    src = (s, slice(None), h * CORES + k, r, slice(None), slice(None), cols[q])
                    dst = (slice(None), s, r) + ((y, slice(None)) if s == 0 else (slice(None), x)) + (
                        c, slice(None), cols[q])
                    if (o, oc) == (0, 0):
                        r_ref[dst] = t_ref[src]
                    else:
                        send(t_ref.at[src], r_ref.at[dst], (HOP2, 1, q, r, s), peer(s, False, h, k))

    def product1(r):
        for q in range(HALVES):
            arrived(HOP2, 1, q, r)
        blk = 2 * LANES
        per = blk // rows
        for s in range(2):
            for ib in range(n // blk):
                for jb in range(n // blk):
                    prod = dot(rf[0, s, r, :, ib * blk:(ib + 1) * blk], rf[1, s, r, :, jb * blk:(jb + 1) * blk], 0, 0)
                    for t in range(2):
                        w = jb * 2 + t
                        xf[s, r, ib * per:(ib + 1) * per, w * rows:(w + 1) * rows, :] = (
                            prod[:, t * LANES:(t + 1) * LANES].reshape(per, rows, LANES))

    def back1(q, r):
        for o in range(1, ny):
            for s in range(2):
                h = (pos2[s] + o) % size2[s]
                src = x_ref.at[s, r, h, :, :, xcols[q]] if s == 0 else x_ref.at[s, r, :, h, :, xcols[q]]
                send(src, u_ref.at[s, :, :, pos2[s], r, xcols[q]], (BACK1, 1, q, r, s), peer(s, False, h, c))
        for s in range(2):
            u_ref[s, :, :, pos2[s], r, xcols[q]] = x_ref[s, r, y, :, :, xcols[q]] if s == 0 else (
                x_ref[s, r, :, x, :, xcols[q]])

    def back2(q, r):
        arrived(BACK1, 1, q, r)
        for o in range(nx):
            for oc in range(CORES):
                for s in range(2):
                    g, k = (pos1[s] + o) % size1[s], (c + oc) % CORES
                    src, dst = (s, g, k, slice(None), r, xcols[q]), (1, s, pos1[s], slice(None), c, r, xcols[q])
                    if (o, oc) == (0, 0):
                        xr_ref[dst] = u_ref[src]
                    else:
                        send(u_ref.at[src], xr_ref.at[dst], (BACK2, 1, q, r, s), peer(s, True, g, k))

    def incoming():
        for q in range(HALVES):
            for r in range(2):
                hop2(q, r)
        left(BACK2, 0)
        for r in range(2):
            product1(r)
            back1(0, r)
        for q in range(1, HALVES):
            for r in range(2):
                back1(q, r)
        for q in range(HALVES):
            for r in range(2):
                back2(q, r)

    stores = []
    for u in range(3):
        for q in range(HALVES):
            if u > 0:
                for r in range(2):
                    arrived(BACK2, u - 1, q, r)
            else:
                loads[q].wait()
            if u == 1 and q == 0:
                left(HOP1, 0)

            @pl.loop(0, rows, unroll=4)
            def _(i):
                if u > 0:
                    finish_row(u - 1, q, i)
                if u < 2:
                    project_row(u, q, i)

            if u == 2:
                c_ = pl.ds(q * width, width)
                stores.append(pltpu.make_async_copy(z_ref.at[:, c_], out_hbm.at[:, c_], zsem.at[1, q]))
                stores[q].start()
                continue
            repack(q)
            if u == 0 and q == 0:
                pl.semaphore_wait(barrier, greeted)
            if u == 0:
                spread(q)
            else:
                for r in range(2):
                    hop1(q, r)
        if u == 0:
            outgoing()
        elif u == 1:
            incoming()
    for stage, u in ((HOP1, 1), (HOP2, 0), (HOP2, 1), (BACK1, 0), (BACK1, 1), (BACK2, 1)):
        left(stage, u)
    for q in range(HALVES):
        stores[q].wait()


def solution(mesh):
    ny, nx = mesh.shape['dap2'], mesh.shape['dap'] // CORES
    assert ny == nx == RING
    g = nx

    def local_step(pair, mask, norm_gain, norm_bias, w_proj, w_gate, post_gain, post_bias, w_out):
        rows, n, ch = pair.shape
        nt = n // LANES
        assert ch == g * g * CORES * 4 and ch == LANES
        vmem = pl.BlockSpec(memory_space=pltpu.VMEM)
        hbm = pl.BlockSpec(memory_space=pl.ANY)
        dma = pltpu.SemaphoreType.DMA
        return pl.pallas_call(
            functools.partial(both_updates, ny, nx),
            name='triangle',
            out_shape=jax.ShapeDtypeStruct(pair.shape, F32),
            in_specs=[hbm] + [vmem] * 8,
            out_specs=hbm,
            scratch_shapes=[
                pltpu.VMEM((rows, n, ch), F32),
                pltpu.VMEM((rows, n, ch), BF16),
                pltpu.VMEM((2, 4 * ch, ch), BF16),
                pltpu.VMEM((2, 2, ch, LANES), F32),
                pltpu.VMEM((2, nt // HALVES, rows * (ch + PAD), LANES), F32),
                pltpu.VMEM((2, 2, g, g * CORES, 2, rows, n), BF16),
                pltpu.VMEM((2, ch // (2 * g * CORES), g * CORES, rows, n), BF16),
                pltpu.VMEM((2, ch // (2 * g * CORES), ny, nx, CORES, rows, n), BF16),
                pltpu.VMEM((2, 2, g * CORES, 2, g, rows, n), BF16),
                pltpu.VMEM((2, 2, 2, ny, nx, CORES, rows, n), BF16),
                pltpu.VMEM((2, 2, ny, nx, CORES, nt * rows, LANES), F32),
                pltpu.VMEM((2, g, CORES, g, 2, nt * rows, LANES), F32),
                pltpu.VMEM((2, 2, g, g, CORES, 2, nt * rows + PAD, LANES), F32),
                dma((4, 2, HALVES, 2, 2)), dma((4, 2, HALVES, 2, 2)), dma((2, HALVES)),
            ],
            compiler_params=pltpu.CompilerParams(collective_id=0, has_side_effects=True,
                                                 vmem_limit_bytes=63 * 2 ** 20),
        )(pair, mask, norm_gain, norm_bias, w_proj, w_gate, post_gain, post_bias, w_out)

    return jax.shard_map(local_step, mesh=mesh, in_specs=(ROW_SPEC, MASK_SPEC) + (P(),) * 7, out_specs=ROW_SPEC,
                         check_vma=False)
```

```python
import functools

import jax
import jax.numpy as jnp
from jax import lax
from jax.experimental import pallas as pl
from jax.experimental.pallas import tpu as pltpu
from jax.sharding import PartitionSpec as P

NORM_EPS = 1e-5
ROW_SPEC = P(('data', 'dap2', 'dap'), None, None)
MASK_SPEC = P(('data', 'dap2', 'dap'), None)
MESH = pl.DeviceIdType.MESH
F32, BF16 = jnp.float32, jnp.bfloat16
CORES = 2
LANES = 128
PAD = 8
HALVES = 2
RING = 4


def norm(values, gain, bias, axis):
    mean = jnp.mean(values, axis=axis, keepdims=True)
    centered = values - mean
    var = jnp.mean(centered * centered, axis=axis, keepdims=True)
    return (centered * lax.rsqrt(var + NORM_EPS) * gain + bias).astype(BF16)


def dot(a, b, ca, cb):
    return lax.dot_general(a, b, (((ca,), (cb,)), ((), ())), preferred_element_type=F32)


def both_updates(ny, nx, z_hbm, mask_ref, ng_ref, nb_ref, wp_ref, wg_ref, pg_ref, pb_ref, wo_ref, z_ref,
                 yn_ref, wt_ref, gb_ref, st_ref, ab_ref, a0_ref, b0_ref, t_ref, r_ref, x_ref, u_ref, xr_ref,
                 ssem, rsem, zsem):
    rows, n, ch = z_ref.shape
    width = n // HALVES
    nt = width // LANES
    xrows = nt * rows
    spad = ch + PAD
    xpad = HALVES * xrows + PAD
    y = lax.axis_index('dap2')
    d = lax.axis_index('dap')
    x, c = d // CORES, d % CORES
    size1, size2 = (nx, ny), (ny, nx)
    pos1, pos2 = (x, y), (y, x)
    blocks = ny * nx * CORES

    loads = []
    for q in range(HALVES):
        cols = pl.ds(q * width, width)
        loads.append(pltpu.make_async_copy(z_hbm.at[:, cols], z_ref.at[:, cols], zsem.at[0, q]))
        loads[q].start()

    def peer(s, first, place, core):
        on_x = (s == 0) == first
        return {'dap2': y, 'dap': place * CORES + core} if on_x else {'dap2': place, 'dap': x * CORES + core}

    barrier = pltpu.get_barrier_semaphore()
    greeted = 0
    for on_x, size, pos in ((True, nx, x), (False, ny, y)):
        for o in range(size):
            for oc in range(CORES):
                if (o, oc) == (0, 0) or (o == 0 and not on_x):
                    continue
                pl.semaphore_signal(barrier, inc=1, device_id=peer(0, on_x, (pos + o) % size, (c + oc) % CORES),
                                    device_id_type=MESH)
                greeted += 1

    for u in range(2):
        wt_ref[u] = wp_ref[u].T
        gb_ref[u, 0] = jnp.broadcast_to(pg_ref[u:u + 1].astype(F32), (LANES, ch)).T
        gb_ref[u, 1] = jnp.broadcast_to(pb_ref[u:u + 1].astype(F32), (LANES, ch)).T

    abf = ab_ref.reshape(2, ch, rows, n)
    rf = r_ref.reshape(2, 2, 2, n, n)
    rw = r_ref.reshape(2, 2, 2, blocks, rows, n)
    band = nx * CORES
    per0 = ch // (2 * band)
    part = per0 // 2
    ab0 = ab_ref.reshape(2, 2, nx, CORES, per0, rows, n)
    a0f = a0_ref.reshape(2, per0, band * rows, n)
    b0f = b0_ref.reshape(2, per0, n, n)
    x0 = x_ref.reshape(2, per0, band, HALVES * xrows, LANES)
    xr0 = xr_ref.reshape(2, 2, nx, CORES, per0, xpad, LANES)
    xf = x_ref.reshape(2, 2, blocks, HALVES * xrows, LANES)
    xrf = xr_ref.reshape(2 * ch * xpad, LANES)

    def finish_row(u, q, i):
        for t in range(nt):
            js = slice(q * width + t * LANES, q * width + (t + 1) * LANES)
            xn = norm(xrf[pl.ds(u * ch * xpad + (q * nt + t) * rows + i, ch, stride=xpad)], gb_ref[u, 0], gb_ref[u, 1], 0)
            upd = dot(xn, wo_ref[u], 0, 0)
            pre = dot(yn_ref[i, js], wg_ref[u], 1, 0)
            z_ref[i, js] = z_ref[i, js] + jax.nn.sigmoid(pre) * upd

    def project_row(u, q, i):
        js = slice(q * width, (q + 1) * width)
        yn = norm(z_ref[i, js], ng_ref[u:u + 1].astype(F32), nb_ref[u:u + 1].astype(F32), -1)
        yn_ref[i, js] = yn
        keep = mask_ref[pl.ds(i, 1), js].astype(F32)
        for side in range(2):
            pr = dot(wt_ref[u, side * 2 * ch:(side + 1) * 2 * ch], yn, 1, 1)
            val = keep * jax.nn.sigmoid(pr[ch:]) * pr[:ch]
            for t in range(nt):
                st_ref[side, t, pl.ds(pl.multiple_of(i * spad, 8), ch)] = val[:, t * LANES:(t + 1) * LANES]

    def repack(q):
        @pl.loop(0, ch, unroll=8)
        def _(k):
            for side in range(2):
                for t in range(nt):
                    lanes = slice(q * width + t * LANES, q * width + (t + 1) * LANES)
                    abf[side, k, :, lanes] = st_ref[side, t, pl.ds(k, rows, stride=spad)].astype(BF16)

    def send(src, dst, where, dev):
        pltpu.make_async_remote_copy(src_ref=src, dst_ref=dst, send_sem=ssem.at[where], recv_sem=rsem.at[where],
                                     device_id=dev, device_id_type=MESH).start()

    def wait(sem, view):
        pltpu.make_async_copy(view, view, sem).wait()

    HOP1, HOP2, BACK1, BACK2 = range(4)
    cols = [slice(q * width, (q + 1) * width) for q in range(HALVES)]
    xcols = [slice(q * xrows, (q + 1) * xrows) for q in range(HALVES)]

    def view(stage, u, q, r, s):
        if u == 0:
            if stage == HOP1:
                return abf.at[:, 0:(band - 1) * per0, :, cols[q]]
            if stage == HOP2:
                return b0_ref.at[s, :, 0, :, :, :, cols[q]]
            if stage == BACK1:
                return b0_ref.at[s, 0:part, 0, :, :, :, cols[q]]
            return x0.at[s, 0:part, 0:band - 1, xcols[q]]
        if stage == HOP1:
            return t_ref.at[s, :, :, r, 0:size1[s] - 1, :, cols[q]]
        if stage == HOP2:
            return rw.at[:, s, r, 0:blocks - blocks // (size2[s] * CORES), :, cols[q]]
        if stage == BACK1:
            return xf.at[s, r, 0:blocks - blocks // size2[s], xcols[q]]
        return xf.at[s, r, 0:blocks - blocks // (size1[s] * CORES), xcols[q]]

    def arrived(stage, u, q, r):
        for s in range(2):
            wait(rsem.at[stage, u, q, r, s], view(stage, u, q, r, s))

    def left(stage, u):
        for q in range(HALVES):
            for r in range(1 if (stage, u) == (HOP1, 0) else 2):
                for s in range(2):
                    wait(ssem.at[stage, u, q, r, s], view(stage, u, q, r, s))

    def slab(s, kk, h, q):
        place = (h, slice(None)) if s == 0 else (slice(None), h)
        return (s, kk) + place + (slice(None), slice(None), cols[q])

    def spread(q):
        for o in range(nx):
            for oc in range(CORES):
                for s in range(2):
                    g, k = (pos1[s] + o) % size1[s], (c + oc) % CORES
                    mine = pos1[s] * CORES + c
                    for side, dst, at in ((1, b0_ref, (s, slice(None), y, x, c, slice(None), cols[q])),
                                          (0, a0_ref, (s, slice(None), mine, slice(None), cols[q]))):
                        src = (side, s, g, k, slice(None), slice(None), cols[q])
                        if (o, oc) == (0, 0):
                            dst[at] = ab0[src]
                        else:
                            send(ab0.at[src], dst.at[at], (HOP1, 0, q, 0, s), peer(s, True, g, k))

    def gather(q, r):
        for step in (1, -1):
            for s in range(2):
                at = slab(s, slice(r * part, (r + 1) * part), pos2[s], q)
                send(b0_ref.at[at], b0_ref.at[at], (HOP2, 0, q, r, s), peer(s, False, (pos2[s] + step) % size2[s], c))

    def relay(q, r):
        arrived(HOP2, 0, q, r)
        half = part // 2
        for step, lo in ((1, 0), (-1, half)):
            for s in range(2):
                at = slab(s, slice(r * part + lo, r * part + lo + half), (pos2[s] - step) % size2[s], q)
                send(b0_ref.at[at], b0_ref.at[at], (BACK1, 0, q, r, s), peer(s, False, (pos2[s] + step) % size2[s], c))

    def product0(r):
        for q in range(HALVES):
            arrived(BACK1, 0, q, r)
        blk = 2 * LANES
        for s in range(2):
            for k in range(r * part, (r + 1) * part):
                for jb in range(n // blk):
                    prod = dot(a0f[s, k], b0f[s, k, jb * blk:(jb + 1) * blk], 1, 1)
                    for t in range(2):
                        w = jb * 2 + t
                        x0[s, k, :, w * rows:(w + 1) * rows, :] = (
                            prod[:, t * LANES:(t + 1) * LANES].reshape(band, rows, LANES))

    def give_back(q, r):
        for o in range(nx):
            for oc in range(CORES):
                for s in range(2):
                    g, k = (pos1[s] + o) % size1[s], (c + oc) % CORES
                    kk = slice(r * part, (r + 1) * part)
                    src, dst = (s, kk, g * CORES + k, xcols[q]), (0, s, pos1[s], c, kk, xcols[q])
                    if (o, oc) == (0, 0):
                        xr0[dst] = x0[src]
                    else:
                        send(x0.at[src], xr0.at[dst], (BACK2, 0, q, r, s), peer(s, True, g, k))

    def outgoing():
        for q in range(HALVES):
            arrived(HOP1, 0, q, 0)
            for r in range(2):
                if (q, r) != (HALVES - 1, 1):
                    gather(q, r)
        for q in range(HALVES):
            relay(q, 0)
        gather(HALVES - 1, 1)
        for q in range(HALVES - 1):
            relay(q, 1)
        product0(0)
        relay(HALVES - 1, 1)
        give_back(0, 0)
        product0(1)
        give_back(0, 1)
        for q in range(1, HALVES):
            for r in range(2):
                give_back(q, r)

    def hop1(q, r):
        for o in range(1, nx):
            for s in range(2):
                g = (pos1[s] + o) % size1[s]
                send(ab_ref.at[:, s, g, :, r, :, cols[q]], t_ref.at[s, :, :, r, pos1[s], :, cols[q]],
                     (HOP1, 1, q, r, s), peer(s, True, g, c))
        for s in range(2):
            t_ref[s, :, :, r, pos1[s], :, cols[q]] = ab_ref[:, s, pos1[s], :, r, :, cols[q]]

    def hop2(q, r):
        arrived(HOP1, 1, q, r)
        for o in range(ny):
            for oc in range(CORES):
                for s in range(2):
                    h, k = (pos2[s] + o) % size2[s], (c + oc) % CORES
                    src = (s, slice(None), h * CORES + k, r, slice(None), slice(None), cols[q])
                    dst = (slice(None), s, r) + ((y, slice(None)) if s == 0 else (slice(None), x)) + (
                        c, slice(None), cols[q])
                    if (o, oc) == (0, 0):
                        r_ref[dst] = t_ref[src]
                    else:
                        send(t_ref.at[src], r_ref.at[dst], (HOP2, 1, q, r, s), peer(s, False, h, k))

    def product1(r):
        for q in range(HALVES):
            arrived(HOP2, 1, q, r)
        blk = 2 * LANES
        per = blk // rows
        for s in range(2):
            for ib in range(n // blk):
                for jb in range(n // blk):
                    prod = dot(rf[0, s, r, :, ib * blk:(ib + 1) * blk], rf[1, s, r, :, jb * blk:(jb + 1) * blk], 0, 0)
                    for t in range(2):
                        w = jb * 2 + t
                        xf[s, r, ib * per:(ib + 1) * per, w * rows:(w + 1) * rows, :] = (
                            prod[:, t * LANES:(t + 1) * LANES].reshape(per, rows, LANES))

    def back1(q, r):
        for o in range(1, ny):
            for s in range(2):
                h = (pos2[s] + o) % size2[s]
                src = x_ref.at[s, r, h, :, :, xcols[q]] if s == 0 else x_ref.at[s, r, :, h, :, xcols[q]]
                send(src, u_ref.at[s, :, :, pos2[s], r, xcols[q]], (BACK1, 1, q, r, s), peer(s, False, h, c))
        for s in range(2):
            u_ref[s, :, :, pos2[s], r, xcols[q]] = x_ref[s, r, y, :, :, xcols[q]] if s == 0 else (
                x_ref[s, r, :, x, :, xcols[q]])

    def back2(q, r):
        arrived(BACK1, 1, q, r)
        for o in range(nx):
            for oc in range(CORES):
                for s in range(2):
                    g, k = (pos1[s] + o) % size1[s], (c + oc) % CORES
                    src, dst = (s, g, k, slice(None), r, xcols[q]), (1, s, pos1[s], slice(None), c, r, xcols[q])
                    if (o, oc) == (0, 0):
                        xr_ref[dst] = u_ref[src]
                    else:
                        send(u_ref.at[src], xr_ref.at[dst], (BACK2, 1, q, r, s), peer(s, True, g, k))

    def incoming():
        for q in range(HALVES):
            for r in range(2):
                hop2(q, r)
        left(BACK2, 0)
        for r in range(2):
            product1(r)
            back1(0, r)
        for q in range(1, HALVES):
            for r in range(2):
                back1(q, r)
        for q in range(HALVES):
            for r in range(2):
                back2(q, r)

    for u in range(3):
        for q in range(HALVES):
            if u > 0:
                for r in range(2):
                    arrived(BACK2, u - 1, q, r)
            else:
                loads[q].wait()
            if u == 1 and q == 0:
                left(HOP1, 0)

            @pl.loop(0, rows, unroll=4)
            def _(i):
                if u > 0:
                    finish_row(u - 1, q, i)
                if u < 2:
                    project_row(u, q, i)

            if u == 2:
                continue
            repack(q)
            if u == 0 and q == 0:
                pl.semaphore_wait(barrier, greeted)
            if u == 0:
                spread(q)
            else:
                for r in range(2):
                    hop1(q, r)
        if u == 0:
            outgoing()
        elif u == 1:
            incoming()
    for stage, u in ((HOP1, 1), (HOP2, 0), (HOP2, 1), (BACK1, 0), (BACK1, 1), (BACK2, 1)):
        left(stage, u)


def solution(mesh):
    ny, nx = mesh.shape['dap2'], mesh.shape['dap'] // CORES
    assert ny == nx == RING
    g = nx

    def local_step(pair, mask, norm_gain, norm_bias, w_proj, w_gate, post_gain, post_bias, w_out):
        rows, n, ch = pair.shape
        nt = n // LANES
        assert ch == g * g * CORES * 4 and ch == LANES
        vmem = pl.BlockSpec(memory_space=pltpu.VMEM)
        hbm = pl.BlockSpec(memory_space=pl.ANY)
        dma = pltpu.SemaphoreType.DMA
        return pl.pallas_call(
            functools.partial(both_updates, ny, nx),
            name='triangle',
            out_shape=pltpu.VMEM(pair.shape, F32),
            in_specs=[hbm] + [vmem] * 8,
            out_specs=vmem,
            scratch_shapes=[
                pltpu.VMEM((rows, n, ch), BF16),
                pltpu.VMEM((2, 4 * ch, ch), BF16),
                pltpu.VMEM((2, 2, ch, LANES), F32),
                pltpu.VMEM((2, nt // HALVES, rows * (ch + PAD), LANES), F32),
                pltpu.VMEM((2, 2, g, g * CORES, 2, rows, n), BF16),
                pltpu.VMEM((2, ch // (2 * g * CORES), g * CORES, rows, n), BF16),
                pltpu.VMEM((2, ch // (2 * g * CORES), ny, nx, CORES, rows, n), BF16),
                pltpu.VMEM((2, 2, g * CORES, 2, g, rows, n), BF16),
                pltpu.VMEM((2, 2, 2, ny, nx, CORES, rows, n), BF16),
                pltpu.VMEM((2, 2, ny, nx, CORES, nt * rows, LANES), F32),
                pltpu.VMEM((2, g, CORES, g, 2, nt * rows, LANES), F32),
                pltpu.VMEM((2, 2, g, g, CORES, 2, nt * rows + PAD, LANES), F32),
                dma((4, 2, HALVES, 2, 2)), dma((4, 2, HALVES, 2, 2)), dma((1, HALVES)),
            ],
            compiler_params=pltpu.CompilerParams(collective_id=0, has_side_effects=True,
                                                 vmem_limit_bytes=56 * 2 ** 20),
        )(pair, mask, norm_gain, norm_bias, w_proj, w_gate, post_gain, post_bias, w_out)

    return jax.shard_map(local_step, mesh=mesh, in_specs=(ROW_SPEC, MASK_SPEC) + (P(),) * 7, out_specs=ROW_SPEC,
                         check_vma=False)
```
